512 devices in a mesh: tx: 32 (over z_lo, y, core), ty: 16 (over z_hi, x).
Axes of the slice: x: 4, y: 8, z: 8 (z_hi: 4, z_lo: 2; z = z_hi * 2 + z_lo), core: 2. Of those that a mesh axis runs over, the one named last changes fastest.
Arguments:
- nodes: bfloat16 [256, 256, 512], P('tx', 'ty'), may hold values from -6 to 6
- edges: bfloat16 [32, 16, 1024, 512], P('tx', 'ty'), may hold values from -6 to 6
- edge_sender: int32 [32, 16, 1024], P('tx', 'ty'), may hold values from 0 to 224, as said below
- edge_receiver: int32 [32, 16, 1024], P('tx', 'ty'), may hold values from 0 to 128, as said below
- coarse_place: int32 [2560], P(('tx', 'ty')), may hold values from 0 to 127, as said below
- edge_w1: bfloat16 [1536, 512], replicated, may hold values from -0.15625 to 0.15625
- edge_w2: bfloat16 [512, 512], replicated, may hold values from -0.25 to 0.25
- edge_gain: float32 [512], replicated, may hold values from 0.1 to 1.9
- node_w1: bfloat16 [1024, 512], replicated, may hold values from -0.1875 to 0.1875
- node_w2: bfloat16 [512, 512], replicated, may hold values from -0.25 to 0.25
- node_gain: float32 [512], replicated, may hold values from 0.1 to 1.9
Outputs:
- new_nodes: bfloat16 [256, 256, 512], P('tx', 'ty')
- new_edges: bfloat16 [32, 16, 1024, 512], P('tx', 'ty')
The draws below stay inside these ranges and needn't reach their ends.
Inputs may be any that keep to these rules, and one draw needn't show every extreme that they name: `edge_sender`: entries below 180 index the tile extended by one node on each side, wrapping around the grid, row-major over (10) x (18); entries from 180 on name a coarse node of the tile or of one of the eight tiles around it, as the steps say. `edge_receiver`: entry 128 marks an empty slot; on each tile the live slots come first, and at least three quarters of the slots are live. A live slot whose sender entry is 180 or more has as receiver one of the tile's own coarse nodes. `coarse_place`: the 5 entries of one tile are distinct.
All inputs are finite; a program needn't handle non-finite values.
Results may differ from the reference program's by a relative error of at most 0.0056.
Values may be sent and summed in bfloat16 or wider, within the bound.
No kernel may reach another device: no remote copies, remote signals or barrier semaphores. Data moves between devices by JAX's collectives and lax.ppermute only.
A program may use at most 64 MiB of HBM per device.

```python
import jax
import jax.numpy as jnp
from jax import lax

D = 512
TILE_X = 8
TILE_Y = 16
EDGE_DEV = 1024
COARSE_DEV = 5
GX = 256
GY = 256
N_TX = 32
N_TY = 16


def draw_graph(key):
    row_span = TILE_Y + 2
    framed = (TILE_X + 2) * row_span
    node_count = TILE_X * TILE_Y
    tiles = N_TX * N_TY
    array_shape = (N_TX, N_TY, EDGE_DEV)
    keys = jax.random.split(jax.random.fold_in(key, 29), 9)
    scores = jax.random.randint(keys[0], (tiles, node_count), 0, 1 << 20)
    scores = scores * node_count + lax.broadcasted_iota(jnp.int32, (tiles, node_count), 1)
    place = jnp.argsort(scores, axis=1, stable=True)[:, :COARSE_DEV].astype(jnp.int32)
    place_grid = place.reshape(N_TX, N_TY, COARSE_DEV)
    category = jax.random.randint(keys[1], array_shape, 0, 10)
    inner_a = jax.random.randint(keys[2], array_shape, 1, TILE_X + 1)
    inner_b = jax.random.randint(keys[3], array_shape, 1, TILE_Y + 1)
    border_pick = jax.random.randint(keys[4], array_shape, 0, 2 * row_span + 2 * TILE_X)
    coarse_pick = jax.random.randint(keys[5], array_shape, 0, 9 * COARSE_DEV)
    interior = inner_a * row_span + inner_b
    side_pick = border_pick - 2 * row_span
    side_cell = (1 + side_pick // 2) * row_span + side_pick % 2 * (TILE_Y + 1)
    bottom_cell = (TILE_X + 1) * row_span + (border_pick - row_span)
    border = jnp.where(border_pick < row_span, border_pick, jnp.where(border_pick < 2 * row_span, bottom_cell, side_cell))
    is_coarse = category >= 8
    sender = jnp.where(is_coarse, framed + coarse_pick, jnp.where(category < 5, interior, border)).astype(jnp.int32)
    owned_pick = jax.random.randint(keys[6], array_shape, 0, COARSE_DEV)
    owned = jnp.take_along_axis(place_grid, owned_pick, axis=2)
    targets = jax.random.randint(keys[7], array_shape, 0, node_count)
    receiver = jnp.where(is_coarse, owned, targets)
    live_count = jax.random.randint(keys[8], (N_TX, N_TY, 1), (3 * EDGE_DEV + 3) // 4, EDGE_DEV + 1)
    slot_index = lax.broadcasted_iota(jnp.int32, array_shape, 2)
    receiver = jnp.where(slot_index < live_count, receiver, node_count).astype(jnp.int32)
    return (sender, receiver, place.reshape(-1))


def draw_edge_sender(key, part):
    return draw_graph(key)[0]


def draw_edge_receiver(key, part):
    return draw_graph(key)[1]


def draw_coarse_place(key, part):
    return draw_graph(key)[2]


def block_scale(own_key, shape, pieces, smallest, top_value):
    def one(axis_at, blocks):
        heights = jax.random.uniform(jax.random.fold_in(jax.random.fold_in(own_key, 6), axis_at), (blocks,), jnp.float32, smallest / len(pieces), top_value / len(pieces))
        return jnp.repeat(jnp.exp(heights), shape[axis_at] // blocks).reshape((-1,) + (1,) * (len(shape) - axis_at - 1))

    factor_of = one(*pieces[0])
    for cut in pieces[1:]:
        factor_of = factor_of * one(*cut)
    return factor_of


def gaussian(key, extent, deviation, most, pieces=(), kind=jnp.bfloat16):
    factor_of = block_scale(key, extent, pieces, -0.22, 0.18) if pieces else 1.0
    values = jax.random.normal(key, extent, jnp.float32) * deviation * factor_of
    return jnp.minimum(jnp.maximum(values, -most), most).astype(kind)


def setup_inputs(seed: int = 0) -> dict:
    streams_of = jax.random.split(jax.random.key(seed), 12)
    nodes = gaussian(streams_of[0], (GX, GY, D), 1.0, 6.0, ((0, 32), (1, 16)))
    edges = gaussian(streams_of[1], (N_TX, N_TY, EDGE_DEV, D), 1.0, 6.0, ((0, 32), (1, 16)))
    edge_sender = draw_edge_sender(jax.random.fold_in(streams_of[11], 71), 0)
    edge_receiver = draw_edge_receiver(jax.random.fold_in(streams_of[11], 71), 0)
    coarse_place = draw_coarse_place(jax.random.fold_in(streams_of[11], 71), 0)
    edge_w1 = gaussian(streams_of[5], (3 * D, D), (3 * D) ** -0.5, 0.15625)
    edge_w2 = gaussian(streams_of[6], (D, D), D ** -0.5, 0.25)
    edge_gain = jnp.clip(1.0 + 0.18 * jax.random.normal(streams_of[7], (D,), jnp.float32), 0.1, 1.9)
    node_w1 = gaussian(streams_of[8], (2 * D, D), (2 * D) ** -0.5, 0.1875)
    node_w2 = gaussian(streams_of[9], (D, D), D ** -0.5, 0.25)
    node_gain = jnp.clip(1.0 + 0.18 * jax.random.normal(streams_of[10], (D,), jnp.float32), 0.1, 1.9)
    return dict(nodes=nodes, edges=edges, edge_sender=edge_sender, edge_receiver=edge_receiver, coarse_place=coarse_place, edge_w1=edge_w1, edge_w2=edge_w2, edge_gain=edge_gain, node_w1=node_w1, node_w2=node_w2, node_gain=node_gain)


eps = 1e-05

def layer_norm(values, gain):
    average = lax.optimization_barrier(jnp.mean(values, -1, keepdims=True))
    centred = values - average
    variance = lax.optimization_barrier(jnp.mean(centred * centred, -1, keepdims=True))
    return centred * lax.rsqrt(variance + eps) * gain

def reference(nodes, edges, edge_sender, edge_receiver, coarse_place, edge_w1, edge_w2, edge_gain, node_w1, node_w2, node_gain):
    feature = nodes.shape[-1]
    node_flat = nodes.reshape(-1, feature)
    sender_term = jnp.dot(node_flat, edge_w1[feature:2 * feature], preferred_element_type=jnp.float32).astype(jnp.bfloat16).reshape(GX, GY, feature)
    receiver_term = jnp.dot(node_flat, edge_w1[2 * feature:], preferred_element_type=jnp.float32).astype(jnp.bfloat16).reshape(GX, GY, feature)
    node_rows = TILE_X * TILE_Y
    row_span = TILE_Y + 2
    framed = (TILE_X + 2) * row_span

    def one_device(device):
        row_block = device // N_TY
        col_block = device % N_TY
        senders = edge_sender[row_block, col_block]
        receivers = edge_receiver[row_block, col_block]
        edge_block = edges[row_block, col_block]
        offset = jnp.clip(senders - framed, 0, 9 * COARSE_DEV - 1)
        window = offset // COARSE_DEV
        member = offset % COARSE_DEV
        owner_x = (row_block + window // 3 - 1) % N_TX
        owner_y = (col_block + window % 3 - 1) % N_TY
        coarse_id = ((owner_x * N_TY + owner_y) * COARSE_DEV + member).astype(jnp.int32)
        position = coarse_place[coarse_id]
        coarse_x = owner_x * TILE_X + position // TILE_Y
        coarse_y = owner_y * TILE_Y + position % TILE_Y
        halo_x = (row_block * TILE_X + senders // row_span - 1) % GX
        halo_y = (col_block * TILE_Y + senders % row_span - 1) % GY
        is_coarse = senders >= framed
        grid_x = jnp.where(is_coarse, coarse_x, halo_x).astype(jnp.int32)
        grid_y = jnp.where(is_coarse, coarse_y, halo_y).astype(jnp.int32)
        picked = sender_term[grid_x, grid_y].astype(jnp.float32)
        is_live = receivers < node_rows
        local_recv = jnp.minimum(receivers, node_rows - 1).astype(jnp.int32)
        recv_x = (row_block * TILE_X + local_recv // TILE_Y).astype(jnp.int32)
        recv_y = (col_block * TILE_Y + local_recv % TILE_Y).astype(jnp.int32)
        recv_rows = receiver_term[recv_x, recv_y].astype(jnp.float32)
        recv_rows = jnp.where(is_live[:, None], recv_rows, jnp.float32(0.0))
        preact = jnp.dot(edge_block, edge_w1[:feature], preferred_element_type=jnp.float32) + picked + recv_rows
        hidden = jax.nn.silu(preact).astype(jnp.bfloat16)
        message = jnp.dot(hidden, edge_w2, preferred_element_type=jnp.float32)
        normed = jnp.where(is_live[:, None], layer_norm(message, edge_gain), jnp.float32(0.0))
        updated = (edge_block.astype(jnp.float32) + normed).astype(jnp.bfloat16)
        contrib = jnp.where(is_live[:, None], updated.astype(jnp.float32), jnp.float32(0.0))
        summed = jax.ops.segment_sum(contrib, local_recv, num_segments=node_rows)
        return (updated, summed.astype(jnp.bfloat16))
    updated, summed = lax.map(one_device, jnp.arange(N_TX * N_TY, dtype=jnp.int32))
    new_edges = updated.reshape(N_TX, N_TY, EDGE_DEV, feature)
    summed = summed.reshape(N_TX, N_TY, TILE_X, TILE_Y, feature).transpose(0, 2, 1, 3, 4).reshape(-1, feature)
    node_pre = jnp.dot(node_flat, node_w1[:feature], preferred_element_type=jnp.float32) + jnp.dot(summed, node_w1[feature:], preferred_element_type=jnp.float32)
    node_hidden = jax.nn.silu(node_pre).astype(jnp.bfloat16)
    node_out = jnp.dot(node_hidden, node_w2, preferred_element_type=jnp.float32)
    new_nodes = (node_flat.astype(jnp.float32) + layer_norm(node_out, node_gain)).astype(jnp.bfloat16)
    return (new_nodes.reshape(GX, GY, feature), new_edges)
```

```python
import functools

import jax
import jax.numpy as jnp
from jax import lax
from jax.experimental import pallas as pl
from jax.experimental.pallas import tpu as pltpu
from jax.sharding import PartitionSpec as P

eps = 1e-05
bf16 = jnp.bfloat16
f32 = jnp.float32
i32 = jnp.int32


def near_pairs(size):
    return [(i, i ^ 1) for i in range(size)]


def far_pairs(size):
    return [(i, (i + 1) % size if i % 2 else (i - 1) % size) for i in range(size)]


def dot(a, b):
    return jnp.dot(a, b, preferred_element_type=f32)


def silu(v):
    return v / (1.0 + jnp.exp(-v))


def normed(values, gain, keep=None):
    average = jnp.mean(values, -1, keepdims=True)
    centred = values - average
    variance = jnp.mean(centred * centred, -1, keepdims=True)
    scale = lax.rsqrt(variance + eps)
    if keep is not None:
        scale = jnp.where(keep, scale, 0.0)
    return centred * scale * gain


near1, far1, near2, far2, table_rows = 0, 24, 48, 80, 128


def pack_kernel(place_ref, nodes_ref, send_near, send_far, own_near, own_far):
    tile_x, tile_y = 8, 16
    last_row = (tile_x - 1) * tile_y
    odd_x = lax.rem(lax.axis_index("tx"), 2)
    odd_y = lax.rem(lax.axis_index("ty"), 2)
    count = nodes_ref.shape[0]
    row = lax.broadcasted_iota(i32, (80, count), 0)
    lane = lax.broadcasted_iota(i32, (80, count), 1)
    first = jnp.where(row < 24, 0, 24)
    within = row - first
    base = jnp.where(row < 24, last_row * (1 - odd_x), last_row * odd_x)
    border = base + jnp.where(
        within < tile_y, within, jnp.where(within == 21, 0, tile_y - 1)
    )
    side = row - jnp.where(row < 64, 48, 64)
    column = jnp.where(row < 64, (tile_y - 1) * (1 - odd_y), (tile_y - 1) * odd_y)
    edge_node = side * tile_y + column
    wanted = jnp.where(row < 48, border, edge_node)
    slot = jnp.where(row < 48, within - 16, side - 8)
    for k in range(5):
        wanted = jnp.where(slot == k, place_ref[k], wanted)
    pick = jnp.where(wanted == lane, 1.0, 0.0).astype(bf16)
    rows = dot(pick, nodes_ref[...]).astype(bf16)
    send_near[...] = rows[0:24]
    send_far[...] = rows[24:48]
    own_near[...] = rows[48:64]
    own_far[...] = rows[64:80]


def sender_slots(sender, place_ref):
    span = 18
    odd_x = lax.rem(lax.axis_index("tx"), 2)
    odd_y = lax.rem(lax.axis_index("ty"), 2)
    above, below = jnp.where(odd_x == 0, far1, near1), jnp.where(odd_x == 0, near1, far1)
    left, right = jnp.where(odd_y == 0, far2, near2), jnp.where(odd_y == 0, near2, far2)
    above_part, below_part = jnp.where(odd_x == 0, 24, 16), jnp.where(odd_x == 0, 16, 24)
    r = lax.div(sender, span)
    c = sender - r * span
    coarse = sender >= 180
    q = sender - 180
    w = lax.div(q, 5)
    k = q - w * 5
    wx = lax.div(w, 3)
    wy = w - wx * 3
    dx = jnp.where(coarse, wx, jnp.where(r == 0, 0, jnp.where(r == 9, 2, 1)))
    dy = jnp.where(coarse, wy, jnp.where(c == 0, 0, jnp.where(c == 17, 2, 1)))
    own_fine = (r - 1) * 16 + (c - 1)
    own_coarse = jnp.zeros_like(sender)
    for m in range(5):
        own_coarse = jnp.where(k == m, place_ref[m], own_coarse)
    mine = (dx == 1) & (dy == 1)
    own = jnp.where(mine, jnp.where(coarse, own_coarse, own_fine), -1)
    vertical = jnp.where(dx == 0, above, below) + jnp.where(coarse, 16 + k, c - 1)
    side = jnp.where(dy == 0, left, right)
    straight = side + jnp.where(coarse, 8 + k, r - 1)
    corner_part = jnp.where(dx == 0, above_part, below_part)
    corner = side + corner_part + jnp.where(coarse, k, jnp.where(dy == 0, 6, 5))
    away = jnp.where(dy == 1, vertical, jnp.where(dx == 1, straight, corner))
    return own, jnp.where(mine, -1, away)


def as_column(index, r):
    return jnp.broadcast_to(index[r : r + 1, :], (128, 128)).T


def one_hot(column, lane):
    return jnp.where(column == lane, 1.0, 0.0).astype(bf16)


def local_kernel(place_ref, nodes_ref, edges_ref, sender_ref, receiver_ref, w1_ref, node_w1_ref, pre_ref, node_pre_ref):
    feature = nodes_ref.shape[1]
    nodes = nodes_ref[...]
    own, _ = sender_slots(sender_ref[...], place_ref)
    receiver = receiver_ref[...]
    table = jnp.concatenate(
        [
            dot(nodes, w1_ref[feature : 2 * feature, :]).astype(bf16),
            dot(nodes, w1_ref[2 * feature :, :]).astype(bf16),
        ],
        axis=0,
    )
    node_pre_ref[...] = dot(nodes, node_w1_ref[0:feature, :])
    lane = lax.broadcasted_iota(i32, (128, 128), 1)
    for r in range(8):
        pick = jnp.concatenate(
            [one_hot(as_column(own, r), lane), one_hot(as_column(receiver, r), lane)], axis=1
        )
        rows = slice(r * 128, (r + 1) * 128)
        pre_ref[rows, :] = dot(edges_ref[rows, :], w1_ref[0:feature, :]) + dot(pick, table)


def finish_kernel(
    place_ref,
    near1_ref,
    far1_ref,
    near2_ref,
    far2_ref,
    pre_ref,
    node_pre_ref,
    nodes_ref,
    edges_ref,
    sender_ref,
    receiver_ref,
    w1_ref,
    w2_ref,
    edge_gain_ref,
    node_w1_ref,
    node_w2_ref,
    node_gain_ref,
    new_nodes_ref,
    new_edges_ref,
    updated_ref,
    table_ref,
    sems,
):
    feature = nodes_ref.shape[1]
    table_ref[near1:far1, :] = near1_ref[...]
    table_ref[far1:near2, :] = far1_ref[...]
    table_ref[near2:far2, :] = near2_ref[...]
    table_ref[far2 : far2 + 32, :] = far2_ref[...]
    table_ref[far2 + 32 :, :] = jnp.zeros((table_rows - far2 - 32, feature), bf16)
    table = dot(table_ref[...], w1_ref[feature : 2 * feature, :]).astype(bf16)
    _, away = sender_slots(sender_ref[...], place_ref)
    receiver = receiver_ref[...]
    lane = lax.broadcasted_iota(i32, (128, 128), 1)
    level = lax.broadcasted_iota(i32, (128, 128), 0)
    gain = edge_gain_ref[...]
    summed = jnp.zeros((128, feature), f32)
    copies = []
    for r in range(8):
        rows = slice(r * 128, (r + 1) * 128)
        pre = pre_ref[rows, :] + dot(one_hot(as_column(away, r), lane), table)
        hidden = silu(pre).astype(bf16)
        message = dot(hidden, w2_ref[...])
        live = as_column(receiver, r)[:, 0:1] < 128
        updated = (edges_ref[rows, :].astype(f32) + normed(message, gain, live)).astype(bf16)
        updated_ref[rows, :] = updated
        copy = pltpu.make_async_copy(updated_ref.at[rows, :], new_edges_ref.at[rows, :], sems.at[r])
        copy.start()
        copies.append(copy)
        landing = jnp.where(level == receiver[r : r + 1, :], 1.0, 0.0).astype(bf16)
        summed = summed + dot(landing, updated)
    hidden = silu(node_pre_ref[...] + dot(summed.astype(bf16), node_w1_ref[feature:, :])).astype(bf16)
    out = dot(hidden, node_w2_ref[...])
    new_nodes_ref[...] = (
        nodes_ref[...].astype(f32) + normed(out, node_gain_ref[...])
    ).astype(bf16)
    for copy in copies:
        copy.wait()


whole = pl.BlockSpec(memory_space=pltpu.VMEM)
scalars = pl.BlockSpec(memory_space=pltpu.SMEM)
anywhere = pl.BlockSpec(memory_space=pl.ANY)


def shards(sizes, nodes, edges, sender, receiver, place, w1, w2, edge_gain, node_w1, node_w2, node_gain):
    tile_x, tile_y, feature = nodes.shape
    size_x, size_y = sizes
    flat = nodes.reshape(tile_x * tile_y, feature)
    edge_flat = edges.reshape(-1, feature)
    send = sender.reshape(8, 128)
    recv = receiver.reshape(8, 128)
    row = jax.ShapeDtypeStruct((24, feature), bf16)
    col = jax.ShapeDtypeStruct((16, feature), bf16)
    send_near, send_far, own_near, own_far = pl.pallas_call(
        pack_kernel,
        out_shape=(row, row, col, col),
        in_specs=[scalars, whole],
        out_specs=(whole,) * 4,
        cost_estimate=pl.CostEstimate(flops=10_000_000_000, bytes_accessed=200_000, transcendentals=0),
        compiler_params=pltpu.CompilerParams(vmem_limit_bytes=4 << 20),
        name="pack",
    )(place, flat)
    got_far1 = lax.ppermute(send_far, "tx", far_pairs(size_x))
    got_near1 = lax.ppermute(send_near, "tx", near_pairs(size_x))
    pre, node_pre = pl.pallas_call(
        local_kernel,
        out_shape=(
            jax.ShapeDtypeStruct((1024, feature), f32),
            jax.ShapeDtypeStruct((128, feature), f32),
        ),
        in_specs=[scalars] + [whole] * 6,
        out_specs=(whole, whole),
        cost_estimate=pl.CostEstimate(flops=1_000_000_000, bytes_accessed=5_000_000, transcendentals=0),
        compiler_params=pltpu.CompilerParams(vmem_limit_bytes=24 << 20),
        name="local",
    )(place, flat, edge_flat, send, recv, w1, node_w1)
    tail = [got_near1[16:24], got_far1[16:24]]
    got_near2 = lax.ppermute(jnp.concatenate([own_near] + tail, 0), "ty", near_pairs(size_y))
    got_far2 = lax.ppermute(jnp.concatenate([own_far] + tail, 0), "ty", far_pairs(size_y))
    new_nodes, new_edges = pl.pallas_call(
        finish_kernel,
        out_shape=(
            jax.ShapeDtypeStruct((128, feature), bf16),
            jax.ShapeDtypeStruct((1024, feature), bf16),
        ),
        in_specs=[scalars] + [whole] * 16,
        out_specs=(whole, anywhere),
        scratch_shapes=[
            pltpu.VMEM((1024, feature), bf16),
            pltpu.VMEM((table_rows, feature), bf16),
            pltpu.SemaphoreType.DMA((8,)),
        ],
        cost_estimate=pl.CostEstimate(flops=1_100_000_000, bytes_accessed=6_000_000, transcendentals=600_000),
        compiler_params=pltpu.CompilerParams(vmem_limit_bytes=24 << 20),
        name="finish",
    )(
        place,
        got_near1,
        got_far1,
        got_near2,
        got_far2,
        pre,
        node_pre,
        flat,
        edge_flat,
        send,
        recv,
        w1,
        w2,
        edge_gain.reshape(1, feature),
        node_w1,
        node_w2,
        node_gain.reshape(1, feature),
    )
    return new_nodes.reshape(nodes.shape), new_edges.reshape(edges.shape)


def solution(mesh):
    placed = (
        P("tx", "ty", None),
        P("tx", "ty", None, None),
        P("tx", "ty", None),
        P("tx", "ty", None),
        P(("tx", "ty")),
        P(),
        P(),
        P(),
        P(),
        P(),
        P(),
    )
    sizes = (mesh.shape["tx"], mesh.shape["ty"])
    return jax.shard_map(
        functools.partial(shards, sizes),
        mesh=mesh,
        in_specs=placed,
        out_specs=(P("tx", "ty", None), P("tx", "ty", None, None)),
        check_vma=False,
    )
```

```python
import functools

import jax
import jax.numpy as jnp
from jax import lax
from jax.experimental import pallas as pl
from jax.experimental.pallas import tpu as pltpu
from jax.sharding import PartitionSpec as P


eps = 1e-05
bf16 = jnp.bfloat16
f32 = jnp.float32
i32 = jnp.int32


def upward(size):
    return [(i, (i + 1) % size) for i in range(size)]


def downward(size):
    return [((i + 1) % size, i) for i in range(size)]


def near_pairs(size):
    return [(i, i ^ 1) for i in range(size)]


def far_pairs(size):
    return [(i, (i + 1) % size if i % 2 else (i - 1) % size) for i in range(size)]


def dot(a, b):
    return jnp.dot(a, b, preferred_element_type=f32)


def silu_of_half(u):
    return u + u * jnp.tanh(u)


def normed(values, gain, keep=None):
    average = jnp.mean(values, -1, keepdims=True)
    centred = values - average
    variance = jnp.mean(centred * centred, -1, keepdims=True)
    scale = lax.rsqrt(variance + eps)
    if keep is not None:
        scale = jnp.where(keep, scale, 0.0)
    return centred * scale * gain


near1, far1, from_left, from_right, table_rows = 0, 24, 48, 80, 128


def pack_kernel(place_hbm, nodes_hbm, send_near, send_far, own_last, own_first, place_rows, place_ref, nodes_ref, sems):
    copies = [
        pltpu.make_async_copy(nodes_hbm, nodes_ref, sems.at[0]),
        pltpu.make_async_copy(place_hbm, place_ref, sems.at[1]),
    ]
    for copy in copies:
        copy.start()
    tile_x, tile_y = 8, 16
    last_row = (tile_x - 1) * tile_y
    odd_x = lax.rem(lax.axis_index("tx"), 2)
    count = tile_x * tile_y
    row = lax.broadcasted_iota(i32, (80, count), 0)
    lane = lax.broadcasted_iota(i32, (80, count), 1)
    first = jnp.where(row < 24, 0, 24)
    within = row - first
    base = jnp.where(row < 24, last_row * (1 - odd_x), last_row * odd_x)
    border = base + jnp.where(
        within < tile_y, within, jnp.where(within == 21, 0, tile_y - 1)
    )
    side = row - jnp.where(row < 64, 48, 64)
    column = jnp.where(row < 64, tile_y - 1, 0)
    edge_node = side * tile_y + column
    wanted = jnp.where(row < 48, border, edge_node)
    slot = jnp.where(row < 48, within - 16, side - 8)
    for copy in copies:
        copy.wait()
    line = lax.broadcasted_iota(i32, (8, 128), 0)
    spread = jnp.zeros((8, 128), i32)
    for k in range(5):
        wanted = jnp.where(slot == k, place_ref[k], wanted)
        spread = jnp.where(line == k, place_ref[k], spread)
    place_rows[...] = spread
    pick = jnp.where(wanted == lane, 1.0, 0.0).astype(bf16)
    rows = dot(pick, nodes_ref[...]).astype(bf16)
    send_near[...] = rows[0:24]
    send_far[...] = rows[24:48]
    own_last[...] = rows[48:64]
    own_first[...] = rows[64:80]


def sender_slots(sender, place_ref):
    span = 18
    odd_x = lax.rem(lax.axis_index("tx"), 2)
    above, below = jnp.where(odd_x == 0, far1, near1), jnp.where(odd_x == 0, near1, far1)
    above_part, below_part = jnp.where(odd_x == 0, 24, 16), jnp.where(odd_x == 0, 16, 24)
    r = lax.div(sender, span)
    c = sender - r * span
    coarse = sender >= 180
    q = sender - 180
    w = lax.div(q, 5)
    k = q - w * 5
    wx = lax.div(w, 3)
    wy = w - wx * 3
    dx = jnp.where(coarse, wx, jnp.where(r == 0, 0, jnp.where(r == 9, 2, 1)))
    dy = jnp.where(coarse, wy, jnp.where(c == 0, 0, jnp.where(c == 17, 2, 1)))
    own_fine = (r - 1) * 16 + (c - 1)
    own_coarse = jnp.zeros_like(sender)
    for m in range(5):
        own_coarse = jnp.where(k == m, place_ref[m : m + 1, :], own_coarse)
    mine = (dx == 1) & (dy == 1)
    own = jnp.where(mine, jnp.where(coarse, own_coarse, own_fine), -1)
    vertical = jnp.where(dx == 0, above, below) + jnp.where(coarse, 16 + k, c - 1)
    side = jnp.where(dy == 0, from_left, from_right)
    straight = side + jnp.where(coarse, 8 + k, r - 1)
    corner_part = jnp.where(dx == 0, above_part, below_part)
    corner = side + corner_part + jnp.where(coarse, k, jnp.where(dy == 0, 6, 5))
    away = jnp.where(dy == 1, vertical, jnp.where(dx == 1, straight, corner))
    return own, jnp.where(mine, -1, away)


def as_column(index, r):
    return jnp.broadcast_to(index[r : r + 1, :], (128, 128)).T


def one_hot(column, lane):
    return jnp.where(column == lane, 1.0, 0.0).astype(bf16)


def local_kernel(place_ref, nodes_ref, edges_ref, sender_ref, receiver_ref, w1_ref, node_w1_ref, pre_ref, node_pre_ref, pick_ref, landing_ref):
    feature = nodes_ref.shape[1]
    nodes = nodes_ref[...]
    own, away = sender_slots(sender_ref[...], place_ref)
    receiver = receiver_ref[...]
    table = jnp.concatenate(
        [
            dot(nodes, w1_ref[feature : 2 * feature, :]).astype(bf16),
            dot(nodes, w1_ref[2 * feature :, :]).astype(bf16),
        ],
        axis=0,
    )
    node_pre_ref[...] = 0.5 * dot(nodes, node_w1_ref[0:feature, :])
    lane = lax.broadcasted_iota(i32, (128, 128), 1)
    for r in range(4):
        pick = jnp.concatenate(
            [
                jnp.concatenate([one_hot(as_column(own, 2 * r + t), lane) for t in range(2)], axis=0),
                jnp.concatenate([one_hot(as_column(receiver, 2 * r + t), lane) for t in range(2)], axis=0),
            ],
            axis=1,
        )
        rows = slice(r * 256, (r + 1) * 256)
        pre_ref[rows, :] = 0.5 * (dot(edges_ref[rows, :], w1_ref[0:feature, :]) + dot(pick, table))
    level = lax.broadcasted_iota(i32, (128, 128), 0)
    for r in range(8):
        rows = slice(r * 128, (r + 1) * 128)
        pick_ref[rows, :] = one_hot(as_column(away, r), lane)
        landing_ref[:, rows] = one_hot(receiver[r : r + 1, :], level)


def finish_kernel(
    near1_ref,
    far1_ref,
    from_left_ref,
    from_right_ref,
    pre_ref,
    node_pre_ref,
    nodes_ref,
    edges_ref,
    pick_ref,
    landing_ref,
    receiver_ref,
    w1_ref,
    w2_ref,
    edge_gain_ref,
    node_w1_ref,
    node_w2_ref,
    node_gain_ref,
    new_nodes_ref,
    new_edges_ref,
    updated_ref,
    table_ref,
    nodes_out_ref,
    sems,
):
    feature = nodes_ref.shape[1]
    table_ref[near1:far1, :] = near1_ref[...]
    table_ref[far1:from_left, :] = far1_ref[...]
    table_ref[from_left:from_right, :] = from_left_ref[...]
    table_ref[from_right : from_right + 32, :] = from_right_ref[...]
    table_ref[from_right + 32 :, :] = jnp.zeros((table_rows - from_right - 32, feature), bf16)
    table = dot(table_ref[...], w1_ref[feature : 2 * feature, :]).astype(bf16) * bf16(0.5)
    receiver = receiver_ref[...]
    live_count = jnp.sum(jnp.where(receiver < 128, 1, 0))
    gain = edge_gain_ref[...]
    summed = jnp.zeros((128, feature), f32)
    copies = []
    for r in range(2):
        rows = slice(r * 512, (r + 1) * 512)
        pre = pre_ref[rows, :] + dot(pick_ref[rows, :], table)
        hidden = silu_of_half(pre).astype(bf16)
        message = dot(hidden, w2_ref[...])
        live = lax.broadcasted_iota(i32, (512, 1), 0) < live_count - 512 * r
        updated = (edges_ref[rows, :].astype(f32) + normed(message, gain, live)).astype(bf16)
        updated_ref[rows, :] = updated
        copy = pltpu.make_async_copy(updated_ref.at[rows, :], new_edges_ref.at[rows, :], sems.at[r])
        copy.start()
        copies.append(copy)
    summed = dot(landing_ref[...], updated_ref[...])
    hidden = silu_of_half(
        node_pre_ref[...] + 0.5 * dot(summed.astype(bf16), node_w1_ref[feature:, :])
    ).astype(bf16)
    out = dot(hidden, node_w2_ref[...])
    for half in range(2):
        rows = slice(half * 64, half * 64 + 64)
        nodes_out_ref[rows, :] = (
            nodes_ref[rows, :].astype(f32) + normed(out[rows, :], node_gain_ref[...])
        ).astype(bf16)
        copy = pltpu.make_async_copy(nodes_out_ref.at[rows, :], new_nodes_ref.at[rows, :], sems.at[6 + half])
        copy.start()
        copies.append(copy)
    for copy in copies:
        copy.wait()


whole = pl.BlockSpec(memory_space=pltpu.VMEM)
scalars = pl.BlockSpec(memory_space=pltpu.SMEM)
anywhere = pl.BlockSpec(memory_space=pl.ANY)


def shards(sizes, *arrays):
    return layer(sizes, *arrays)


def layer(sizes, nodes, edges, sender, receiver, place, w1, w2, edge_gain, node_w1, node_w2, node_gain):
    tile_x, tile_y, feature = nodes.shape
    size_x, size_y = sizes
    flat = nodes.reshape(tile_x * tile_y, feature)
    edge_flat = edges.reshape(-1, feature)
    send = sender.reshape(8, 128)
    recv = receiver.reshape(8, 128)
    row = jax.ShapeDtypeStruct((24, feature), bf16)
    col = jax.ShapeDtypeStruct((16, feature), bf16)
    send_near, send_far, own_last, own_first, place_rows = pl.pallas_call(
        pack_kernel,
        out_shape=(row, row, col, col, jax.ShapeDtypeStruct((8, 128), i32)),
        in_specs=[pl.BlockSpec(memory_space=pltpu.HBM)] * 2,
        out_specs=(whole,) * 5,
        scratch_shapes=[
            pltpu.SMEM((5,), i32),
            pltpu.VMEM((128, feature), bf16),
            pltpu.SemaphoreType.DMA((2,)),
        ],
        cost_estimate=pl.CostEstimate(flops=10_000_000_000, bytes_accessed=200_000, transcendentals=0),
        compiler_params=pltpu.CompilerParams(vmem_limit_bytes=4 << 20),
        name="pack",
    )(
        pltpu.with_memory_space_constraint(place, pltpu.HBM),
        pltpu.with_memory_space_constraint(flat, pltpu.HBM),
    )
    got_far1 = lax.ppermute(send_far, "tx", far_pairs(size_x))
    got_near1 = lax.ppermute(send_near, "tx", near_pairs(size_x))
    pre, node_pre, pick, landing = pl.pallas_call(
        local_kernel,
        out_shape=(
            jax.ShapeDtypeStruct((1024, feature), f32),
            jax.ShapeDtypeStruct((128, feature), f32),
            jax.ShapeDtypeStruct((1024, table_rows), bf16),
            jax.ShapeDtypeStruct((128, 1024), bf16),
        ),
        in_specs=[whole] * 7,
        out_specs=(whole,) * 4,
        cost_estimate=pl.CostEstimate(flops=1_000_000_000, bytes_accessed=5_000_000, transcendentals=0),
        compiler_params=pltpu.CompilerParams(vmem_limit_bytes=24 << 20),
        name="local",
    )(place_rows, flat, edge_flat, send, recv, w1, node_w1)
    tail = [got_near1[16:24], got_far1[16:24]]
    got_from_left = lax.ppermute(jnp.concatenate([own_last] + tail, 0), "ty", upward(size_y))
    got_from_right = lax.ppermute(jnp.concatenate([own_first] + tail, 0), "ty", downward(size_y))
    new_nodes, new_edges = pl.pallas_call(
        finish_kernel,
        out_shape=(
            jax.ShapeDtypeStruct((128, feature), bf16),
            jax.ShapeDtypeStruct((1024, feature), bf16),
        ),
        in_specs=[whole] * 17,
        out_specs=(anywhere, anywhere),
        scratch_shapes=[
            pltpu.VMEM((1024, feature), bf16),
            pltpu.VMEM((table_rows, feature), bf16),
            pltpu.VMEM((128, feature), bf16),
            pltpu.SemaphoreType.DMA((8,)),
        ],
        cost_estimate=pl.CostEstimate(flops=1_100_000_000, bytes_accessed=6_000_000, transcendentals=600_000),
        compiler_params=pltpu.CompilerParams(vmem_limit_bytes=24 << 20),
        name="finish",
    )(
        got_near1,
        got_far1,
        got_from_left,
        got_from_right,
        pre,
        node_pre,
        flat,
        edge_flat,
        pick,
        landing,
        recv,
        w1,
        w2,
        edge_gain.reshape(1, feature),
        node_w1,
        node_w2,
        node_gain.reshape(1, feature),
    )
    return new_nodes.reshape(nodes.shape), new_edges.reshape(edges.shape)


def solution(mesh):
    placed = (
        P("tx", "ty", None),
        P("tx", "ty", None, None),
        P("tx", "ty", None),
        P("tx", "ty", None),
        P(("tx", "ty")),
        P(),
        P(),
        P(),
        P(),
        P(),
        P(),
    )
    sizes = (mesh.shape["tx"], mesh.shape["ty"])
    return jax.shard_map(
        functools.partial(shards, sizes),
        mesh=mesh,
        in_specs=placed,
        out_specs=(P("tx", "ty", None), P("tx", "ty", None, None)),
        check_vma=False,
    )
```

```python
import functools

import jax
import jax.numpy as jnp
from jax import lax
from jax.experimental import pallas as pl
from jax.experimental.pallas import tpu as pltpu
from jax.sharding import PartitionSpec as P


eps = 1e-05
bf16 = jnp.bfloat16
f32 = jnp.float32
i32 = jnp.int32


def upward(size):
    return [(i, (i + 1) % size) for i in range(size)]


def downward(size):
    return [((i + 1) % size, i) for i in range(size)]


def far_pairs(size):
    return [(i, (i + 1) % size if i % 2 else (i - 1) % size) for i in range(size)]


def dot(a, b):
    return jnp.dot(a, b, preferred_element_type=f32)


def silu_of_half(u):
    return u + u * jnp.tanh(u)


def normed(values, gain, keep=None):
    average = jnp.mean(values, -1, keepdims=True)
    centred = values - average
    variance = jnp.mean(centred * centred, -1, keepdims=True)
    scale = lax.rsqrt(variance + eps)
    if keep is not None:
        scale = jnp.where(keep, scale, 0.0)
    return centred * scale * gain


near1, far1, from_left, from_right, table_rows = 0, 24, 48, 80, 128


def pack_kernel(place_hbm, nodes_hbm, send_near, send_far, own_last, own_first, place_rows, place_ref, nodes_ref, sems):
    copies = [
        pltpu.make_async_copy(nodes_hbm, nodes_ref, sems.at[0]),
        pltpu.make_async_copy(place_hbm, place_ref, sems.at[1]),
    ]
    for copy in copies:
        copy.start()
    tile_x, tile_y = 8, 16
    last_row = (tile_x - 1) * tile_y
    odd_x = lax.rem(lax.axis_index("tx"), 2)
    count = tile_x * tile_y
    row = lax.broadcasted_iota(i32, (80, count), 0)
    lane = lax.broadcasted_iota(i32, (80, count), 1)
    first = jnp.where(row < 24, 0, 24)
    within = row - first
    base = jnp.where(row < 24, last_row * (1 - odd_x), last_row * odd_x)
    border = base + jnp.where(
        within < tile_y, within, jnp.where(within == 21, 0, tile_y - 1)
    )
    side = row - jnp.where(row < 64, 48, 64)
    column = jnp.where(row < 64, tile_y - 1, 0)
    edge_node = side * tile_y + column
    wanted = jnp.where(row < 48, border, edge_node)
    slot = jnp.where(row < 48, within - 16, side - 8)
    for copy in copies:
        copy.wait()
    line = lax.broadcasted_iota(i32, (8, 128), 0)
    spread = jnp.zeros((8, 128), i32)
    for k in range(5):
        wanted = jnp.where(slot == k, place_ref[k], wanted)
        spread = jnp.where(line == k, place_ref[k], spread)
    place_rows[...] = spread
    pick = jnp.where(wanted == lane, 1.0, 0.0).astype(bf16)
    rows = dot(pick, nodes_ref[...]).astype(bf16)
    send_near[...] = rows[0:24]
    send_far[...] = rows[24:48]
    own_last[...] = rows[48:64]
    own_first[...] = rows[64:80]


def sender_slots(sender, place_ref):
    span = 18
    odd_x = lax.rem(lax.axis_index("tx"), 2)
    above, below = jnp.where(odd_x == 0, far1, near1), jnp.where(odd_x == 0, near1, far1)
    above_part, below_part = jnp.where(odd_x == 0, 24, 16), jnp.where(odd_x == 0, 16, 24)
    r = lax.div(sender, span)
    c = sender - r * span
    coarse = sender >= 180
    q = sender - 180
    w = lax.div(q, 5)
    k = q - w * 5
    wx = lax.div(w, 3)
    wy = w - wx * 3
    dx = jnp.where(coarse, wx, jnp.where(r == 0, 0, jnp.where(r == 9, 2, 1)))
    dy = jnp.where(coarse, wy, jnp.where(c == 0, 0, jnp.where(c == 17, 2, 1)))
    own_fine = (r - 1) * 16 + (c - 1)
    own_coarse = jnp.zeros_like(sender)
    for m in range(5):
        own_coarse = jnp.where(k == m, place_ref[m : m + 1, :], own_coarse)
    mine = (dx == 1) & (dy == 1)
    own = jnp.where(mine, jnp.where(coarse, own_coarse, own_fine), -1)
    vertical = jnp.where(dx == 0, above, below) + jnp.where(coarse, 16 + k, c - 1)
    side = jnp.where(dy == 0, from_left, from_right)
    straight = side + jnp.where(coarse, 8 + k, r - 1)
    corner_part = jnp.where(dx == 0, above_part, below_part)
    corner = side + corner_part + jnp.where(coarse, k, jnp.where(dy == 0, 6, 5))
    away = jnp.where(dy == 1, vertical, jnp.where(dx == 1, straight, corner))
    return own, jnp.where(mine, -1, away)


def as_column(index, r):
    return jnp.broadcast_to(index[r : r + 1, :], (128, 128)).T


def one_hot(column, lane):
    return jnp.where(column == lane, 1.0, 0.0).astype(bf16)


def local_kernel(place_ref, nodes_ref, edges_ref, sender_ref, receiver_ref, w1_ref, pre_ref, pick_ref, landing_ref):
    feature = nodes_ref.shape[1]
    nodes = nodes_ref[...]
    own, away = sender_slots(sender_ref[...], place_ref)
    receiver = receiver_ref[...]
    table = jnp.concatenate(
        [
            dot(nodes, w1_ref[feature : 2 * feature, :]).astype(bf16),
            dot(nodes, w1_ref[2 * feature :, :]).astype(bf16),
        ],
        axis=0,
    )
    lane = lax.broadcasted_iota(i32, (128, 128), 1)
    for r in range(4):
        pick = jnp.concatenate(
            [
                jnp.concatenate([one_hot(as_column(own, 2 * r + t), lane) for t in range(2)], axis=0),
                jnp.concatenate([one_hot(as_column(receiver, 2 * r + t), lane) for t in range(2)], axis=0),
            ],
            axis=1,
        )
        rows = slice(r * 256, (r + 1) * 256)
        pre_ref[rows, :] = 0.5 * (dot(edges_ref[rows, :], w1_ref[0:feature, :]) + dot(pick, table))
    level = lax.broadcasted_iota(i32, (128, 128), 0)
    for r in range(8):
        rows = slice(r * 128, (r + 1) * 128)
        pick_ref[rows, :] = one_hot(as_column(away, r), lane)
        landing_ref[:, rows] = one_hot(receiver[r : r + 1, :], level)


def finish_kernel(
    near1_ref,
    far1_ref,
    from_left_ref,
    from_right_ref,
    pre_ref,
    nodes_ref,
    edges_ref,
    pick_ref,
    landing_ref,
    receiver_ref,
    w1_ref,
    w2_ref,
    edge_gain_ref,
    node_w1_hbm,
    node_w2_hbm,
    node_gain_ref,
    new_nodes_ref,
    new_edges_ref,
    updated_ref,
    table_ref,
    nodes_out_ref,
    node_w1_ref,
    node_w2_ref,
    sems,
    weight_sems,
):
    feature = nodes_ref.shape[1]
    weights = [
        pltpu.make_async_copy(node_w1_hbm, node_w1_ref, weight_sems.at[0]),
        pltpu.make_async_copy(node_w2_hbm, node_w2_ref, weight_sems.at[1]),
    ]
    for copy in weights:
        copy.start()
    table_ref[near1:far1, :] = jnp.where(
        lax.rem(lax.axis_index("tx"), 2) == 0, near1_ref[24:48, :], near1_ref[0:24, :]
    )
    table_ref[far1:from_left, :] = far1_ref[...]
    table_ref[from_left:from_right, :] = from_left_ref[...]
    table_ref[from_right : from_right + 32, :] = from_right_ref[...]
    table_ref[from_right + 32 :, :] = jnp.zeros((table_rows - from_right - 32, feature), bf16)
    table = dot(table_ref[...], w1_ref[feature : 2 * feature, :]).astype(bf16) * bf16(0.5)
    receiver = receiver_ref[...]
    live_count = jnp.sum(jnp.where(receiver < 128, 1, 0))
    gain = edge_gain_ref[...]
    summed = jnp.zeros((128, feature), f32)
    copies = []
    for r in range(2):
        rows = slice(r * 512, (r + 1) * 512)
        pre = pre_ref[rows, :] + dot(pick_ref[rows, :], table)
        hidden = silu_of_half(pre).astype(bf16)
        message = dot(hidden, w2_ref[...])
        live = lax.broadcasted_iota(i32, (512, 1), 0) < live_count - 512 * r
        updated = (edges_ref[rows, :].astype(f32) + normed(message, gain, live)).astype(bf16)
        updated_ref[rows, :] = updated
        copy = pltpu.make_async_copy(updated_ref.at[rows, :], new_edges_ref.at[rows, :], sems.at[r])
        copy.start()
        copies.append(copy)
    summed = dot(landing_ref[...], updated_ref[...])
    for copy in weights:
        copy.wait()
    hidden = silu_of_half(
        0.5
        * (
            dot(nodes_ref[...], node_w1_ref[0:feature, :])
            + dot(summed.astype(bf16), node_w1_ref[feature:, :])
        )
    ).astype(bf16)
    out = dot(hidden, node_w2_ref[...])
    for half in range(2):
        rows = slice(half * 64, half * 64 + 64)
        nodes_out_ref[rows, :] = (
            nodes_ref[rows, :].astype(f32) + normed(out[rows, :], node_gain_ref[...])
        ).astype(bf16)
        copy = pltpu.make_async_copy(nodes_out_ref.at[rows, :], new_nodes_ref.at[rows, :], sems.at[6 + half])
        copy.start()
        copies.append(copy)
    for copy in copies:
        copy.wait()


whole = pl.BlockSpec(memory_space=pltpu.VMEM)
scalars = pl.BlockSpec(memory_space=pltpu.SMEM)
anywhere = pl.BlockSpec(memory_space=pl.ANY)
in_hbm = pl.BlockSpec(memory_space=pltpu.HBM)


def shards(sizes, *arrays):
    return layer(sizes, *arrays)


def layer(sizes, nodes, edges, sender, receiver, place, w1, w2, edge_gain, node_w1, node_w2, node_gain):
    node_w1 = pltpu.with_memory_space_constraint(node_w1, pltpu.HBM)
    node_w2 = pltpu.with_memory_space_constraint(node_w2, pltpu.HBM)
    tile_x, tile_y, feature = nodes.shape
    size_x, size_y = sizes
    flat = nodes.reshape(tile_x * tile_y, feature)
    edge_flat = edges.reshape(-1, feature)
    send = sender.reshape(8, 128)
    recv = receiver.reshape(8, 128)
    row = jax.ShapeDtypeStruct((24, feature), bf16)
    col = jax.ShapeDtypeStruct((16, feature), bf16)
    send_near, send_far, own_last, own_first, place_rows = pl.pallas_call(
        pack_kernel,
        out_shape=(row, row, col, col, jax.ShapeDtypeStruct((8, 128), i32)),
        in_specs=[pl.BlockSpec(memory_space=pltpu.HBM)] * 2,
        out_specs=(whole,) * 5,
        scratch_shapes=[
            pltpu.SMEM((5,), i32),
            pltpu.VMEM((128, feature), bf16),
            pltpu.SemaphoreType.DMA((2,)),
        ],
        cost_estimate=pl.CostEstimate(flops=10_000_000_000, bytes_accessed=200_000, transcendentals=0),
        compiler_params=pltpu.CompilerParams(vmem_limit_bytes=4 << 20),
        name="pack",
    )(
        pltpu.with_memory_space_constraint(place, pltpu.HBM),
        pltpu.with_memory_space_constraint(flat, pltpu.HBM),
    )
    got_far1 = lax.ppermute(send_far, "tx", far_pairs(size_x))
    pair = lax.all_gather(
        send_near, "tx", axis_index_groups=[[i, i + 1] for i in range(0, size_x, 2)], tiled=True
    )
    tails = jnp.where(lax.axis_index("tx") % 2 == 0, pair[40:48], pair[16:24])
    pre, pick, landing = pl.pallas_call(
        local_kernel,
        out_shape=(
            jax.ShapeDtypeStruct((1024, feature), f32),
            jax.ShapeDtypeStruct((1024, table_rows), bf16),
            jax.ShapeDtypeStruct((128, 1024), bf16),
        ),
        in_specs=[whole] * 6,
        out_specs=(whole,) * 3,
        cost_estimate=pl.CostEstimate(flops=1_000_000_000, bytes_accessed=5_000_000, transcendentals=0),
        compiler_params=pltpu.CompilerParams(vmem_limit_bytes=24 << 20),
        name="local",
    )(place_rows, flat, edge_flat, send, recv, w1)
    tail = [tails, got_far1[16:24]]
    got_from_left = lax.ppermute(jnp.concatenate([own_last] + tail, 0), "ty", upward(size_y))
    got_from_right = lax.ppermute(jnp.concatenate([own_first] + tail, 0), "ty", downward(size_y))
    new_nodes, new_edges = pl.pallas_call(
        finish_kernel,
        out_shape=(
            jax.ShapeDtypeStruct((128, feature), bf16),
            jax.ShapeDtypeStruct((1024, feature), bf16),
        ),
        in_specs=[whole] * 13 + [in_hbm] * 2 + [whole],
        out_specs=(anywhere, anywhere),
        scratch_shapes=[
            pltpu.VMEM((1024, feature), bf16),
            pltpu.VMEM((table_rows, feature), bf16),
            pltpu.VMEM((128, feature), bf16),
            pltpu.VMEM((2 * feature, feature), bf16),
            pltpu.VMEM((feature, feature), bf16),
            pltpu.SemaphoreType.DMA((8,)),
            pltpu.SemaphoreType.DMA((2,)),
        ],
        cost_estimate=pl.CostEstimate(flops=1_100_000_000, bytes_accessed=6_000_000, transcendentals=600_000),
        compiler_params=pltpu.CompilerParams(vmem_limit_bytes=24 << 20),
        name="finish",
    )(
        pair,
        got_far1,
        got_from_left,
        got_from_right,
        pre,
        flat,
        edge_flat,
        pick,
        landing,
        recv,
        w1,
        w2,
        edge_gain.reshape(1, feature),
        node_w1,
        node_w2,
        node_gain.reshape(1, feature),
    )
    return new_nodes.reshape(nodes.shape), new_edges.reshape(edges.shape)


def solution(mesh):
    placed = (
        P("tx", "ty", None),
        P("tx", "ty", None, None),
        P("tx", "ty", None),
        P("tx", "ty", None),
        P(("tx", "ty")),
        P(),
        P(),
        P(),
        P(),
        P(),
        P(),
    )
    sizes = (mesh.shape["tx"], mesh.shape["ty"])
    return jax.shard_map(
        functools.partial(shards, sizes),
        mesh=mesh,
        in_specs=placed,
        out_specs=(P("tx", "ty", None), P("tx", "ty", None, None)),
        check_vma=False,
    )
```

```python
import functools

import jax
import jax.numpy as jnp
from jax import lax
from jax.experimental import pallas as pl
from jax.experimental.pallas import tpu as pltpu
from jax.sharding import PartitionSpec as P


eps = 1e-05
bf16 = jnp.bfloat16
f32 = jnp.float32
i32 = jnp.int32


def upward(size):
    return [(i, (i + 1) % size) for i in range(size)]


def downward(size):
    return [((i + 1) % size, i) for i in range(size)]


def far_pairs(size):
    return [(i, (i + 1) % size if i % 2 else (i - 1) % size) for i in range(size)]


def dot(a, b):
    return jnp.dot(a, b, preferred_element_type=f32)


def silu_of_half(u):
    return u + u * jnp.tanh(u)


def normed(values, gain, keep=None):
    average = jnp.mean(values, -1, keepdims=True)
    centred = values - average
    variance = jnp.mean(centred * centred, -1, keepdims=True)
    scale = lax.rsqrt(variance + eps)
    if keep is not None:
        scale = jnp.where(keep, scale, 0.0)
    return centred * scale * gain


near1, far1, from_left, from_right, table_rows = 0, 24, 48, 80, 128


def pack_kernel(place_hbm, nodes_hbm, send_near, send_far, own_last, own_first, place_rows, place_ref, nodes_ref, sems):
    copies = [pltpu.make_async_copy(place_hbm, place_ref, sems.at[4])]
    for n in range(4):
        some = slice(n * 32, (n + 1) * 32)
        copies.append(
            pltpu.make_async_copy(nodes_hbm.at[some, :], nodes_ref.at[some, :], sems.at[n])
        )
    for copy in copies:
        copy.start()
    tile_x, tile_y = 8, 16
    last_row = (tile_x - 1) * tile_y
    odd_x = lax.rem(lax.axis_index("tx"), 2)
    count = tile_x * tile_y
    row = lax.broadcasted_iota(i32, (80, count), 0)
    lane = lax.broadcasted_iota(i32, (80, count), 1)
    first = jnp.where(row < 24, 0, 24)
    within = row - first
    base = jnp.where(row < 24, last_row * (1 - odd_x), last_row * odd_x)
    border = base + jnp.where(
        within < tile_y, within, jnp.where(within == 21, 0, tile_y - 1)
    )
    side = row - jnp.where(row < 64, 48, 64)
    column = jnp.where(row < 64, tile_y - 1, 0)
    edge_node = side * tile_y + column
    wanted = jnp.where(row < 48, border, edge_node)
    slot = jnp.where(row < 48, within - 16, side - 8)
    for copy in copies:
        copy.wait()
    line = lax.broadcasted_iota(i32, (8, 128), 0)
    spread = jnp.zeros((8, 128), i32)
    for k in range(5):
        wanted = jnp.where(slot == k, place_ref[k], wanted)
        spread = jnp.where(line == k, place_ref[k], spread)
    place_rows[...] = spread
    pick = jnp.where(wanted == lane, 1.0, 0.0).astype(bf16)
    rows = dot(pick, nodes_ref[...]).astype(bf16)
    send_near[...] = rows[0:24]
    send_far[...] = rows[24:48]
    own_last[...] = rows[48:64]
    own_first[...] = rows[64:80]


def sender_slots(sender, place_ref):
    span = 18
    odd_x = lax.rem(lax.axis_index("tx"), 2)
    above, below = jnp.where(odd_x == 0, far1, near1), jnp.where(odd_x == 0, near1, far1)
    above_part, below_part = jnp.where(odd_x == 0, 24, 16), jnp.where(odd_x == 0, 16, 24)
    r = lax.div(sender, span)
    c = sender - r * span
    coarse = sender >= 180
    q = sender - 180
    w = lax.div(q, 5)
    k = q - w * 5
    wx = lax.div(w, 3)
    wy = w - wx * 3
    dx = jnp.where(coarse, wx, jnp.where(r == 0, 0, jnp.where(r == 9, 2, 1)))
    dy = jnp.where(coarse, wy, jnp.where(c == 0, 0, jnp.where(c == 17, 2, 1)))
    own_fine = (r - 1) * 16 + (c - 1)
    own_coarse = jnp.zeros_like(sender)
    for m in range(5):
        own_coarse = jnp.where(k == m, place_ref[m : m + 1, :], own_coarse)
    mine = (dx == 1) & (dy == 1)
    own = jnp.where(mine, jnp.where(coarse, own_coarse, own_fine), -1)
    vertical = jnp.where(dx == 0, above, below) + jnp.where(coarse, 16 + k, c - 1)
    side = jnp.where(dy == 0, from_left, from_right)
    straight = side + jnp.where(coarse, 8 + k, r - 1)
    corner_part = jnp.where(dx == 0, above_part, below_part)
    corner = side + corner_part + jnp.where(coarse, k, jnp.where(dy == 0, 6, 5))
    away = jnp.where(dy == 1, vertical, jnp.where(dx == 1, straight, corner))
    return own, jnp.where(mine, -1, away)


def as_column(index, r):
    return jnp.broadcast_to(index[r : r + 1, :], (128, 128)).T


def one_hot(column, lane):
    return jnp.where(column == lane, 1.0, 0.0).astype(bf16)


def local_kernel(place_ref, nodes_ref, edges_ref, sender_ref, receiver_ref, w1_ref, pre_ref, pick_ref, landing_ref):
    feature = nodes_ref.shape[1]
    nodes = nodes_ref[...]
    own, away = sender_slots(sender_ref[...], place_ref)
    receiver = receiver_ref[...]
    table = jnp.concatenate(
        [
            dot(nodes, w1_ref[feature : 2 * feature, :]).astype(bf16),
            dot(nodes, w1_ref[2 * feature :, :]).astype(bf16),
        ],
        axis=0,
    )
    lane = lax.broadcasted_iota(i32, (128, 128), 1)
    for r in range(4):
        pick = jnp.concatenate(
            [
                jnp.concatenate([one_hot(as_column(own, 2 * r + t), lane) for t in range(2)], axis=0),
                jnp.concatenate([one_hot(as_column(receiver, 2 * r + t), lane) for t in range(2)], axis=0),
            ],
            axis=1,
        )
        rows = slice(r * 256, (r + 1) * 256)
        pre_ref[rows, :] = 0.5 * (dot(edges_ref[rows, :], w1_ref[0:feature, :]) + dot(pick, table))
    level = lax.broadcasted_iota(i32, (128, 128), 0)
    for r in range(8):
        rows = slice(r * 128, (r + 1) * 128)
        pick_ref[rows, :] = one_hot(as_column(away, r), lane)
        landing_ref[:, rows] = one_hot(receiver[r : r + 1, :], level)


def finish_kernel(
    near1_ref,
    far1_ref,
    from_left_ref,
    from_right_ref,
    pre_ref,
    nodes_ref,
    edges_ref,
    pick_ref,
    landing_ref,
    receiver_ref,
    w1_ref,
    w2_ref,
    edge_gain_ref,
    node_w1_hbm,
    node_w2_hbm,
    node_gain_ref,
    new_nodes_ref,
    new_edges_ref,
    updated_ref,
    table_ref,
    nodes_out_ref,
    node_w1_ref,
    node_w2_ref,
    sems,
    weight_sems,
):
    feature = nodes_ref.shape[1]
    weights = [
        pltpu.make_async_copy(node_w1_hbm.at[0:feature, :], node_w1_ref.at[0:feature, :], weight_sems.at[0]),
        pltpu.make_async_copy(node_w1_hbm.at[feature:, :], node_w1_ref.at[feature:, :], weight_sems.at[2]),
        pltpu.make_async_copy(node_w2_hbm, node_w2_ref, weight_sems.at[1]),
    ]
    for copy in weights:
        copy.start()
    table_ref[near1:far1, :] = jnp.where(
        lax.rem(lax.axis_index("tx"), 2) == 0, near1_ref[24:48, :], near1_ref[0:24, :]
    )
    table_ref[far1:from_left, :] = far1_ref[...]
    table_ref[from_left:from_right, :] = from_left_ref[...]
    table_ref[from_right : from_right + 32, :] = from_right_ref[...]
    table_ref[from_right + 32 :, :] = jnp.zeros((table_rows - from_right - 32, feature), bf16)
    table = dot(table_ref[...], w1_ref[feature : 2 * feature, :]).astype(bf16) * bf16(0.5)
    receiver = receiver_ref[...]
    live_count = jnp.sum(jnp.where(receiver < 128, 1, 0))
    gain = edge_gain_ref[...]
    summed = jnp.zeros((128, feature), f32)
    copies = []
    for r in range(2):
        rows = slice(r * 512, (r + 1) * 512)
        pre = pre_ref[rows, :] + dot(pick_ref[rows, :], table)
        hidden = silu_of_half(pre).astype(bf16)
        message = dot(hidden, w2_ref[...])
        live = lax.broadcasted_iota(i32, (512, 1), 0) < live_count - 512 * r
        updated = (edges_ref[rows, :].astype(f32) + normed(message, gain, live)).astype(bf16)
        updated_ref[rows, :] = updated
        copy = pltpu.make_async_copy(updated_ref.at[rows, :], new_edges_ref.at[rows, :], sems.at[r])
        copy.start()
        copies.append(copy)
    summed = dot(landing_ref[...], updated_ref[...])
    for copy in weights:
        copy.wait()
    hidden = silu_of_half(
        0.5
        * (
            dot(nodes_ref[...], node_w1_ref[0:feature, :])
            + dot(summed.astype(bf16), node_w1_ref[feature:, :])
        )
    ).astype(bf16)
    out = dot(hidden, node_w2_ref[...])
    for half in range(2):
        rows = slice(half * 64, half * 64 + 64)
        nodes_out_ref[rows, :] = (
            nodes_ref[rows, :].astype(f32) + normed(out[rows, :], node_gain_ref[...])
        ).astype(bf16)
        copy = pltpu.make_async_copy(nodes_out_ref.at[rows, :], new_nodes_ref.at[rows, :], sems.at[6 + half])
        copy.start()
        copies.append(copy)
    for copy in copies:
        copy.wait()


whole = pl.BlockSpec(memory_space=pltpu.VMEM)
scalars = pl.BlockSpec(memory_space=pltpu.SMEM)
anywhere = pl.BlockSpec(memory_space=pl.ANY)
in_hbm = pl.BlockSpec(memory_space=pltpu.HBM)


def shards(sizes, *arrays):
    return layer(sizes, *arrays)


def layer(sizes, nodes, edges, sender, receiver, place, w1, w2, edge_gain, node_w1, node_w2, node_gain):
    node_w1 = pltpu.with_memory_space_constraint(node_w1, pltpu.HBM)
    node_w2 = pltpu.with_memory_space_constraint(node_w2, pltpu.HBM)
    tile_x, tile_y, feature = nodes.shape
    size_x, size_y = sizes
    flat = nodes.reshape(tile_x * tile_y, feature)
    edge_flat = edges.reshape(-1, feature)
    send = sender.reshape(8, 128)
    recv = receiver.reshape(8, 128)
    row = jax.ShapeDtypeStruct((24, feature), bf16)
    col = jax.ShapeDtypeStruct((16, feature), bf16)
    send_near, send_far, own_last, own_first, place_rows = pl.pallas_call(
        pack_kernel,
        out_shape=(row, row, col, col, jax.ShapeDtypeStruct((8, 128), i32)),
        in_specs=[pl.BlockSpec(memory_space=pltpu.HBM)] * 2,
        out_specs=(whole,) * 5,
        scratch_shapes=[
            pltpu.SMEM((5,), i32),
            pltpu.VMEM((128, feature), bf16),
            pltpu.SemaphoreType.DMA((5,)),
        ],
        cost_estimate=pl.CostEstimate(flops=10_000_000_000, bytes_accessed=200_000, transcendentals=0),
        compiler_params=pltpu.CompilerParams(vmem_limit_bytes=4 << 20),
        name="pack",
    )(
        pltpu.with_memory_space_constraint(place, pltpu.HBM),
        pltpu.with_memory_space_constraint(flat, pltpu.HBM),
    )
    got_far1 = lax.ppermute(send_far, "tx", far_pairs(size_x))
    pair = lax.all_gather(
        send_near, "tx", axis_index_groups=[[i, i + 1] for i in range(0, size_x, 2)], tiled=True
    )
    tails = jnp.where(lax.axis_index("tx") % 2 == 0, pair[40:48], pair[16:24])
    pre, pick, landing = pl.pallas_call(
        local_kernel,
        out_shape=(
            jax.ShapeDtypeStruct((1024, feature), f32),
            jax.ShapeDtypeStruct((1024, table_rows), bf16),
            jax.ShapeDtypeStruct((128, 1024), bf16),
        ),
        in_specs=[whole] * 6,
        out_specs=(whole,) * 3,
        cost_estimate=pl.CostEstimate(flops=1_000_000_000, bytes_accessed=5_000_000, transcendentals=0),
        compiler_params=pltpu.CompilerParams(vmem_limit_bytes=24 << 20),
        name="local",
    )(place_rows, flat, edge_flat, send, recv, w1)
    tail = [tails, got_far1[16:24]]
    got_from_left = lax.ppermute(jnp.concatenate([own_last] + tail, 0), "ty", upward(size_y))
    got_from_right = lax.ppermute(jnp.concatenate([own_first] + tail, 0), "ty", downward(size_y))
    new_nodes, new_edges = pl.pallas_call(
        finish_kernel,
        out_shape=(
            jax.ShapeDtypeStruct((128, feature), bf16),
            jax.ShapeDtypeStruct((1024, feature), bf16),
        ),
        in_specs=[whole] * 13 + [in_hbm] * 2 + [whole],
        out_specs=(anywhere, anywhere),
        scratch_shapes=[
            pltpu.VMEM((1024, feature), bf16),
            pltpu.VMEM((table_rows, feature), bf16),
            pltpu.VMEM((128, feature), bf16),
            pltpu.VMEM((2 * feature, feature), bf16),
            pltpu.VMEM((feature, feature), bf16),
            pltpu.SemaphoreType.DMA((8,)),
            pltpu.SemaphoreType.DMA((3,)),
        ],
        cost_estimate=pl.CostEstimate(flops=1_100_000_000, bytes_accessed=6_000_000, transcendentals=600_000),
        compiler_params=pltpu.CompilerParams(vmem_limit_bytes=24 << 20),
        name="finish",
    )(
        pair,
        got_far1,
        got_from_left,
        got_from_right,
        pre,
        flat,
        edge_flat,
        pick,
        landing,
        recv,
        w1,
        w2,
        edge_gain.reshape(1, feature),
        node_w1,
        node_w2,
        node_gain.reshape(1, feature),
    )
    return new_nodes.reshape(nodes.shape), new_edges.reshape(edges.shape)


def solution(mesh):
    placed = (
        P("tx", "ty", None),
        P("tx", "ty", None, None),
        P("tx", "ty", None),
        P("tx", "ty", None),
        P(("tx", "ty")),
        P(),
        P(),
        P(),
        P(),
        P(),
        P(),
    )
    sizes = (mesh.shape["tx"], mesh.shape["ty"])
    return jax.shard_map(
        functools.partial(shards, sizes),
        mesh=mesh,
        in_specs=placed,
        out_specs=(P("tx", "ty", None), P("tx", "ty", None, None)),
        check_vma=False,
    )
```
